32 devices in a mesh: sp: 16 (over z, x, core), dp: 2 (over y).
Axes of the slice: x: 2, y: 2, z: 4, core: 2. Of those that a mesh axis runs over, the one named last changes fastest.
Arguments:
- queries: bfloat16 [1536, 24, 128], P(('dp', 'sp')), parts along dimension 0, may hold values from -12 to 12
- keys: bfloat16 [1536, 24, 128], P(('dp', 'sp')), parts along dimension 0, may hold values from -6 to 6
- values: bfloat16 [1536, 24, 128], P(('dp', 'sp')), parts along dimension 0, may hold values from -6 to 6
Outputs:
- attended: bfloat16 [1536, 3072], P(('dp', 'sp')), parts along dimension 0
The draws below stay inside these ranges and needn't reach their ends.
There are 2 independent parts, one for each index of `dp`. The reference program is written for one: setup_inputs(seed, part) draws one part's arguments, and reference() takes and returns one part's arrays. A program takes and returns all parts, laid end to end along the dimension named above; each array names one. Nothing has to cross between parts.
All inputs are finite; a program needn't handle non-finite values.
Results may differ from the reference program's by a relative error of at most 0.0049.
Values may be sent and summed in bfloat16 or wider, within the bound.
A program may use at most 64 MiB of HBM per device.

```python
import jax
import jax.numpy as jnp
from jax import lax

HEADS = 24
HEAD_DIM = 128
SEQ = 768


def draw_queries(key, part):
    own_key = jax.random.fold_in(key, 1)
    result = 2.5 * jax.random.truncated_normal(own_key, -4.8, 4.8, (SEQ, HEADS, HEAD_DIM), jnp.float32)
    return result.astype(jnp.bfloat16)


def draw_keys(key, part):
    own_key = jax.random.fold_in(key, 2)
    result = jax.random.truncated_normal(own_key, -6.0, 6.0, (SEQ, HEADS, HEAD_DIM), jnp.float32)
    return result.astype(jnp.bfloat16)


def levels(rng, extent, pieces, least, largest):
    level, own = 1.0, jax.random.fold_in(rng, 6)
    for position, shards_of in pieces:
        steps = jnp.exp(jax.random.uniform(jax.random.fold_in(own, position), (shards_of,), jnp.float32, least / len(pieces), largest / len(pieces)))
        level = level * jnp.repeat(steps, extent[position] // shards_of).reshape([-1 if axis == position else 1 for axis in range(len(extent))])
    return level


def gaussian(stream_key, shape, scale, bound, pieces=(), dtype=jnp.bfloat16):
    drawn = jax.random.normal(stream_key, shape, jnp.float32) * scale
    if len(pieces) > 0:
        drawn = levels(stream_key, shape, pieces, -0.22, 0.18) * drawn
    return jnp.clip(drawn, min=-bound, max=bound).astype(dtype)


def setup_inputs(seed: int = 0, part: int = 0) -> dict:
    splits = jax.random.split(jax.random.key(seed), 4)
    part_keys = jax.random.split(jax.random.fold_in(splits[3], part), 4)
    return {
        "queries": draw_queries(jax.random.fold_in(jax.random.fold_in(splits[3], part), 71), part),
        "keys": draw_keys(jax.random.fold_in(jax.random.fold_in(splits[3], part), 71), part),
        "values": gaussian(part_keys[2], (SEQ, HEADS, HEAD_DIM), 1.0, 6.0, ((0, 16),)),
    }


def attend(triple):
    head_q, head_k, head_v = triple
    scale = 1.0 / (head_q.shape[-1] ** 0.5)
    scores = jnp.dot(head_q, head_k.T, preferred_element_type=jnp.float32) * scale
    weights = jax.nn.softmax(scores, axis=-1).astype(jnp.bfloat16)
    return jnp.dot(weights, head_v, preferred_element_type=jnp.float32)


def reference(queries, keys, values):
    seq_len, heads, width = queries.shape
    result = lax.map(attend, (queries.transpose(1, 0, 2), keys.transpose(1, 0, 2), values.transpose(1, 0, 2)))
    return result.transpose(1, 0, 2).reshape(seq_len, heads * width).astype(jnp.bfloat16)
```

```python
import functools
import math

import jax
import jax.numpy as jnp
from jax import lax
from jax.experimental import pallas as pl
from jax.experimental.pallas import tpu as pltpu
from jax.sharding import PartitionSpec as P

HGROUPS = 8
COLUMNS = 2
MESH = pl.DeviceIdType.MESH


def order_of(group, groups):
    half = groups // 2
    side = group // half
    far = [(1 - side) * half + lax.rem(group + step, half) for step in range(half)]
    near = [side * half + lax.rem(group + step, half) for step in range(1, half)]
    return far, near


def ranked(group, groups):
    half = groups // 2
    side, place = group // half, lax.rem(group, half)
    far = [(1 - side) * half + step for step in range(half)]
    near = [side * half + step + (step + half - place) // half for step in range(half - 1)]
    return far, near


def kernel(
    groups, blocks, per_group,
    q_hbm, k_hbm, v_hbm, landed,
    raw, wide, send, held, result,
    in_sem, send_sem, recv_sem, pass_sem, took_sem, back_sem, home_sem, known,
):
    me = lax.axis_index("sp")
    group, block = me // blocks, lax.rem(me, blocks)
    tokens, heads, width = q_hbm.shape
    half = groups // 2
    side = group // half
    far, near = order_of(group, groups)
    partners = [lax.rem(block + step, blocks) for step in range(1, blocks)]

    loads = [
        pltpu.make_async_copy(src, raw.at[i], in_sem.at[i])
        for i, src in enumerate((q_hbm, k_hbm, v_hbm))
    ]
    for load in loads:
        load.start()

    rows = groups // COLUMNS
    row, column = group // COLUMNS, lax.rem(group, COLUMNS)
    above, below = row < rows - 1, row > 0
    across = row * COLUMNS + 1 - column

    def at(step, other_column):
        return (row + step) * COLUMNS + other_column

    def greet(semaphore, other):
        pl.semaphore_signal(semaphore, inc=1, device_id={"sp": other * blocks + block}, device_id_type=MESH)

    barrier = pltpu.get_barrier_semaphore()

    @pl.when(below)
    def greet_below():
        greet(barrier, at(-1, column))

    @pl.when(above)
    def greet_above():
        greet(barrier, at(1, column))

    greet(barrier, across)
    for partner in partners:
        pl.semaphore_signal(barrier, inc=1, device_id={"sp": group * blocks + partner}, device_id_type=MESH)

    for i, load in enumerate(loads):
        load.wait()
        wide[i] = raw[i].astype(jnp.float32).reshape(tokens * heads, width)

    def outward(j, other, part):
        return pltpu.make_async_remote_copy(
            src_ref=send.at[other, j],
            dst_ref=held.at[j, block, group],
            send_sem=send_sem,
            recv_sem=recv_sem.at[j, part],
            device_id={"sp": other * blocks + block},
            device_id_type=MESH,
        )

    def own(j):
        return pltpu.make_async_copy(send.at[group, j], held.at[j, block, group], recv_sem.at[j, 0])

    def sources(part):
        return pl.ds((side if part == 0 else 1 - side) * half, half)

    def arrived(j, part):
        whole = held.at[j, block, sources(part)]
        pltpu.make_async_copy(whole, whole, recv_sem.at[j, part]).wait()

    def share(j, part, partner):
        piece = held.at[j, block, sources(part), pl.ds(1, 2)]
        return pltpu.make_async_remote_copy(
            src_ref=piece,
            dst_ref=piece,
            send_sem=pass_sem.at[partner],
            recv_sem=took_sem.at[j, block],
            device_id={"sp": group * blocks + partner},
            device_id_type=MESH,
        )

    def shared(j, partner):
        whole = held.at[j, partner, :, pl.ds(1, 2)]
        pltpu.make_async_copy(whole, whole, took_sem.at[j, partner]).wait()

    def columns(of, j):
        return pl.ds(pl.multiple_of((of * per_group + j) * width, width), width)

    def back(j, other):
        return pltpu.make_async_remote_copy(
            src_ref=result.at[j, other],
            dst_ref=landed.at[:, columns(group, j)],
            send_sem=back_sem,
            recv_sem=home_sem,
            device_id={"sp": other * blocks + block},
            device_id_type=MESH,
        )

    def own_back(j):
        return pltpu.make_async_copy(result.at[j, group], landed.at[:, columns(group, j)], home_sem)

    for j in range(per_group):
        for to in range(groups):
            head = to * per_group + j
            for i in range(3):
                rows_of = wide[i, pl.ds(head, tokens, stride=heads), :]
                send[to, j, i] = rows_of.astype(jnp.bfloat16)

    def send_first(other):
        outward(0, other, jnp.where(other // half == side, 0, 1)).start()

    def tell_below(other):
        @pl.when(below)
        def tell():
            greet(known.at[other], at(-1, column))

    def tell_above(other):
        @pl.when(above)
        def tell():
            greet(known.at[other], at(1, column))

    def tell_across(other):
        greet(known.at[other], across)

    own(0).start()
    pl.semaphore_wait(barrier, blocks + above.astype(jnp.int32) + below.astype(jnp.int32))

    @pl.when(above)
    def know_above():
        other = at(1, column)
        tell_below(other)
        tell_across(other)
        greet(known.at[across], other)

    @pl.when(below)
    def know_below():
        tell_above(at(-1, column))

    for step in range(1, rows):
        @pl.when(row + step < rows)
        def up():
            other = at(step, column)
            if step > 1:
                pl.semaphore_wait(known.at[other], 1)
                tell_below(other)
                tell_across(other)
            send_first(other)

        @pl.when(row - step >= 0)
        def down():
            other = at(-step, column)
            if step > 1:
                pl.semaphore_wait(known.at[other], 1)
                tell_above(other)
            send_first(other)

        if step == 1:
            send_first(across)

        @pl.when(row - step >= 0)
        def down_across():
            other = at(-step, 1 - column)
            pl.semaphore_wait(known.at[other], 1)
            tell_above(other)
            send_first(other)

        @pl.when(row + step < rows)
        def up_across():
            other = at(step, 1 - column)
            pl.semaphore_wait(known.at[other], 1)
            send_first(other)

    for j in range(1, per_group):
        for other in far:
            outward(j, other, 1).start()
        for other in near:
            outward(j, other, 0).start()
        own(j).start()

    factor = math.log2(math.e) / math.sqrt(width)
    far, near = ranked(group, groups)
    for j in range(per_group):
        for part in range(2):
            arrived(j, part)
            for partner in partners:
                share(j, part, partner).start()
        for partner in partners:
            shared(j, partner)
        keys = held[j, :, :, 1].reshape(-1, width)
        values = held[j, :, :, 2].reshape(-1, width)
        if j == per_group - 1:
            @pl.when(side == 0)
            def release():
                for earlier in (1,):
                    for other in far:
                        back(earlier, other).start()

        for first, picked in (((1 - side) * half, far), (side * half, near)):
            queries = held[j, block, pl.ds(first, half), 0].reshape(half * tokens, width)
            scores = lax.dot_general(
                queries, keys, (((1,), (1,)), ((), ())), preferred_element_type=jnp.float32
            )
            top = jnp.max(scores, axis=-1, keepdims=True)
            weights = jnp.exp2((scores - top) * factor)
            total = jnp.sum(weights, axis=-1, keepdims=True)
            attended = jnp.dot(
                weights.astype(jnp.bfloat16), values, preferred_element_type=jnp.float32
            ) / total
            result[j, pl.ds(first, half)] = attended.astype(jnp.bfloat16).reshape(half, tokens, width)
            if picked is far and j in (1,):
                @pl.when(side > 0)
                def forward():
                    for other in picked:
                        back(j, other).start()
            else:
                for other in picked:
                    back(j, other).start()
        own_back(j).start()

    sent = send.at[pl.ds(0, groups - 1)]
    pltpu.make_async_copy(sent, sent, send_sem).wait()
    for partner in partners:
        passed = held.at[:, block, :, pl.ds(1, 2)]
        pltpu.make_async_copy(passed, passed, pass_sem.at[partner]).wait()
    given = result.at[:, pl.ds(0, groups - 1)]
    pltpu.make_async_copy(given, given, back_sem).wait()
    pltpu.make_async_copy(landed, landed, home_sem).wait()


def shards(queries, keys, values):
    tokens, heads, width = queries.shape
    groups = HGROUPS
    blocks = lax.axis_size("sp") // groups
    per_group = heads // groups
    kind = queries.dtype
    return pl.pallas_call(
        functools.partial(kernel, groups, blocks, per_group),
        out_shape=pltpu.VMEM((tokens, heads * width), kind),
        in_specs=[pl.BlockSpec(memory_space=pl.ANY)] * 3,
        out_specs=pl.BlockSpec(memory_space=pltpu.VMEM),
        scratch_shapes=[
            pltpu.VMEM((3, tokens, heads, width), kind),
            pltpu.VMEM((3, tokens * heads, width), jnp.float32),
            pltpu.VMEM((groups, per_group, 3, tokens, width), kind),
            pltpu.VMEM((per_group, blocks, groups, 3, tokens, width), kind),
            pltpu.VMEM((per_group, groups, tokens, width), kind),
            pltpu.SemaphoreType.DMA((3,)),
            pltpu.SemaphoreType.DMA,
            pltpu.SemaphoreType.DMA((per_group, 2)),
            pltpu.SemaphoreType.DMA((blocks,)),
            pltpu.SemaphoreType.DMA((per_group, blocks)),
            pltpu.SemaphoreType.DMA,
            pltpu.SemaphoreType.DMA,
            pltpu.SemaphoreType.REGULAR((groups,)),
        ],
        compiler_params=pltpu.CompilerParams(collective_id=0, has_side_effects=True),
    )(queries, keys, values)


def solution(mesh):
    return jax.shard_map(
        shards,
        mesh=mesh,
        in_specs=(
            P(("dp", "sp"), None, None),
            P(("dp", "sp"), None, None),
            P(("dp", "sp"), None, None),
        ),
        out_specs=P(("dp", "sp"), None),
        check_vma=False,
    )
```

```python
import functools
import math

import jax
import jax.numpy as jnp
from jax import lax
from jax.experimental import pallas as pl
from jax.experimental.pallas import tpu as pltpu
from jax.sharding import PartitionSpec as P

MESH = pl.DeviceIdType.MESH
UNROLLED = 4


def kernel(
    owners, per_owner, size,
    q_hbm, k_hbm, v_hbm, landed,
    raw, wide, send, held, result,
    in_sem, send_sem, recv_sem, query_sem, back_sem, home_sem,
):
    me = lax.axis_index("sp")
    tokens, heads, width = q_hbm.shape
    first, half = (size - owners) // 2, owners // 2
    side = me // (size // 2)
    mine = me - first
    owner = jnp.logical_and(mine >= 0, mine < owners)
    last = per_owner - 1
    chunks = size // half

    loads = [
        pltpu.make_async_copy(src, raw.at[i], in_sem.at[i])
        for i, src in enumerate((k_hbm, v_hbm, q_hbm))
    ]
    for load in loads:
        load.start()

    barrier = pltpu.get_barrier_semaphore()

    @pl.when(owner)
    def greet():
        for step in range(1, size):
            other = lax.rem(me + step, size)
            pl.semaphore_signal(barrier, inc=1, device_id={"sp": other}, device_id_type=MESH)

    for i, load in enumerate(loads):
        load.wait()
        wide[i] = raw[i].astype(jnp.float32).reshape(tokens * heads, width)

    spot = lax.rem(mine + size, half)
    far = [(1 - side) * half + lax.rem(spot + step, half) for step in range(half)]
    near = [side * half + lax.rem(spot + step, half) for step in range(half)]

    def outward(j, to, parts, semaphore):
        return pltpu.make_async_remote_copy(
            src_ref=send.at[j, to, parts],
            dst_ref=held.at[j, me, parts],
            send_sem=send_sem,
            recv_sem=semaphore,
            device_id={"sp": first + to},
            device_id_type=MESH,
        )

    def own(j, parts, semaphore):
        return pltpu.make_async_copy(send.at[j, mine, parts], held.at[j, me, parts], semaphore)

    def spread(j, parts, semaphore, over=True, around=True):
        for step in range(half):
            if over:
                outward(j, far[step], parts, semaphore).start()
            if around and step > 0:
                outward(j, near[step], parts, semaphore).start()
        if around:
            @pl.when(owner)
            def keep():
                own(j, parts, semaphore).start()

            @pl.when(jnp.logical_not(owner))
            def give():
                outward(j, near[0], parts, semaphore).start()

    asking = pl.ds(2, 1), query_sem.at[me // half]

    for j in range(per_owner):
        for to in range(owners):
            head = to * per_owner + j
            for i in range(3):
                rows = wide[i, pl.ds(head, tokens, stride=heads), :]
                send[j, to, i] = rows.astype(jnp.bfloat16)
        if j == 0:
            @pl.when(owner)
            def meet():
                pl.semaphore_wait(barrier, owners - 1)

            @pl.when(jnp.logical_not(owner))
            def see():
                pl.semaphore_wait(barrier, owners)

        if j < last:
            spread(j, pl.ds(0, 3), recv_sem.at[j])

    @pl.when(jnp.logical_not(owner))
    def ask():
        spread(last, *asking)

    spread(last, pl.ds(0, 2), recv_sem.at[last])

    @pl.when(owner)
    def ask_near():
        spread(last, *asking, over=False)

    def columns(j):
        return pl.ds(pl.multiple_of((mine * per_owner + j) * width, width), width)

    def back(j, other):
        return pltpu.make_async_remote_copy(
            src_ref=result.at[j, other],
            dst_ref=landed.at[:, columns(j)],
            send_sem=back_sem,
            recv_sem=home_sem,
            device_id={"sp": other},
            device_id_type=MESH,
        )

    def own_back(j):
        return pltpu.make_async_copy(result.at[j, me], landed.at[:, columns(j)], home_sem)

    factor = math.log2(math.e) / math.sqrt(width)

    middle = chunks // 2

    def chunk_of(place):
        lower = jnp.where(place == 0, 0, jnp.where(place <= chunks - middle, chunks - place, place - chunks + middle))
        upper = jnp.where(place < middle, place, chunks + middle - 1 - place)
        return jnp.where(side > 0, upper, lower)

    def attend(j, place):
        chunk = chunk_of(place)
        picked = pl.ds(chunk * half, half)
        if j == last:
            asked = held.at[j, picked, pl.ds(2, 1)]
            pltpu.make_async_copy(asked, asked, query_sem.at[chunk]).wait()
        keys = held[j, :, 0].reshape(-1, width)
        values = held[j, :, 1].reshape(-1, width)
        queries = held[j, picked, 2].reshape(half * tokens, width)
        scores = lax.dot_general(
            queries, keys, (((1,), (1,)), ((), ())), preferred_element_type=jnp.float32
        )
        top = jnp.max(scores, axis=-1, keepdims=True)
        weights = jnp.exp2((scores - top) * factor)
        total = jnp.sum(weights, axis=-1, keepdims=True)
        attended = jnp.dot(
            weights.astype(jnp.bfloat16), values, preferred_element_type=jnp.float32
        ) / total
        result[j, picked] = attended.astype(jnp.bfloat16).reshape(half, tokens, width)

    def deliver(j, place):
        chunk = chunk_of(place)
        for step in range(half):
            other = chunk * half + step
            if isinstance(place, int) and place < chunks - 1:
                back(j, other).start()
            else:
                @pl.when(other != me)
                def give():
                    back(j, other).start()

    def early(j):
        attend(j, 0)
        deliver(j, 0)
        if j == 0:
            spread(last, *asking, around=False)

    def late(j, place):
        attend(j, place)
        deliver(j, place)

    @pl.when(owner)
    def work():
        for j in range(per_owner):
            whole = held.at[j] if j < last else held.at[j, :, pl.ds(0, 2)]
            pltpu.make_async_copy(whole, whole, recv_sem.at[j]).wait()
            early(j)
            if chunks > UNROLLED:
                pl.loop(1, chunks)(functools.partial(late, j))
            else:
                if j == last and last > 0:
                    deliver(last - 1, 1)
                for place in range(1, chunks):
                    attend(j, place)
                    if place > 1 or j != last - 1:
                        deliver(j, place)
            own_back(j).start()
        sent = send.at[:, pl.ds(0, owners - 1)]
        pltpu.make_async_copy(sent, sent, send_sem).wait()
        given = result.at[:, pl.ds(0, size - 1)]
        pltpu.make_async_copy(given, given, back_sem).wait()

    @pl.when(jnp.logical_not(owner))
    def rest():
        pltpu.make_async_copy(send, send, send_sem).wait()

    pltpu.make_async_copy(landed, landed, home_sem).wait()


def shards(queries, keys, values):
    tokens, heads, width = queries.shape
    size = lax.axis_size("sp")
    owners = math.gcd(heads, size // 2)
    per_owner = heads // owners
    kind = queries.dtype
    return pl.pallas_call(
        functools.partial(kernel, owners, per_owner, size),
        out_shape=pltpu.VMEM((tokens, heads * width), kind),
        in_specs=[pl.BlockSpec(memory_space=pl.ANY)] * 3,
        out_specs=pl.BlockSpec(memory_space=pltpu.VMEM),
        scratch_shapes=[
            pltpu.VMEM((3, tokens, heads, width), kind),
            pltpu.VMEM((3, tokens * heads, width), jnp.float32),
            pltpu.VMEM((per_owner, owners, 3, tokens, width), kind),
            pltpu.VMEM((per_owner, size, 3, tokens, width), kind),
            pltpu.VMEM((per_owner, size, tokens, width), kind),
            pltpu.SemaphoreType.DMA((3,)),
            pltpu.SemaphoreType.DMA,
            pltpu.SemaphoreType.DMA((per_owner,)),
            pltpu.SemaphoreType.DMA((2 * size // owners,)),
            pltpu.SemaphoreType.DMA,
            pltpu.SemaphoreType.DMA,
        ],
        compiler_params=pltpu.CompilerParams(collective_id=0, has_side_effects=True),
    )(queries, keys, values)


def solution(mesh):
    return jax.shard_map(
        shards,
        mesh=mesh,
        in_specs=(
            P(("dp", "sp"), None, None),
            P(("dp", "sp"), None, None),
            P(("dp", "sp"), None, None),
        ),
        out_specs=P(("dp", "sp"), None),
        check_vma=False,
    )
```

```python
import functools
import math

import jax
import jax.numpy as jnp
from jax import lax
from jax.experimental import pallas as pl
from jax.experimental.pallas import tpu as pltpu
from jax.sharding import PartitionSpec as P

MESH = pl.DeviceIdType.MESH
UNROLLED = 4
ALL, PAIR, ASK = pl.ds(0, 3), pl.ds(0, 2), pl.ds(2, 1)


def kernel(
    owners, slots, size,
    q_hbm, k_hbm, v_hbm, landed,
    raw, wide, send, held, result,
    in_sem, send_sem, recv_sem, query_sem, back_sem, home_sem, near_sem,
):
    me = lax.axis_index("sp")
    tokens, _, width = q_hbm.shape
    first, half = (size - owners) // 2, owners // 2
    side = me // (size // 2)
    mine = me - first
    owner = jnp.logical_and(mine >= 0, mine < owners)
    outer = jnp.logical_not(owner)
    last = slots - 1
    chunks = size // half

    def load(j, i, src):
        return pltpu.make_async_copy(
            src.at[:, pl.ds(j * owners, owners), :], raw.at[j, i], in_sem.at[j]
        )

    for j in range(slots):
        for i, src in enumerate((k_hbm, v_hbm, q_hbm)):
            load(j, i, src).start()

    barrier = pltpu.get_barrier_semaphore()

    def greet(semaphore, other):
        pl.semaphore_signal(semaphore, inc=1, device_id={"sp": other}, device_id_type=MESH)

    spot = lax.rem(mine + size, half)
    far = [(1 - side) * half + lax.rem(spot + step, half) for step in range(half)]
    near = [side * half + lax.rem(spot + step, half) for step in range(half)]

    low = side == 0
    mates = range(0, first, half)

    @pl.when(owner)
    def enter():
        for to in far:
            greet(barrier, first + to)
        for other in range(first):
            greet(barrier, size - 1 - other)

        @pl.when(low)
        def enter_low():
            for other in range(first):
                greet(barrier, other)

    @pl.when(jnp.logical_and(outer, low))
    def enter_outer():
        greet(barrier, first + spot)

    def outward(j, to, parts, semaphore):
        return pltpu.make_async_remote_copy(
            src_ref=send.at[j, to, parts],
            dst_ref=held.at[j, me, parts],
            send_sem=send_sem,
            recv_sem=semaphore,
            device_id={"sp": first + to},
            device_id_type=MESH,
        )

    def own(j, parts, semaphore):
        return pltpu.make_async_copy(send.at[j, mine, parts], held.at[j, me, parts], semaphore)

    def asking():
        return query_sem.at[me // half]

    def spread(targets, j, parts, semaphore):
        for to in targets:
            outward(j, to, parts, semaphore).start()

    mixed = [to for pair in zip(far, near) for to in pair]
    crew = jnp.where(owner, half + jnp.where(low, len(mates), 0), jnp.where(low, half, owners))
    for j in range(slots):
        pltpu.make_async_copy(raw.at[j], raw.at[j], in_sem.at[j]).wait()
        for i in range(3):
            wide[j, i] = raw[j, i].astype(jnp.float32).reshape(tokens * owners, width)
        for to in range(owners):
            for i in range(3):
                rows = wide[j, i, pl.ds(to, tokens, stride=owners), :]
                send[j, to, i] = rows.astype(jnp.bfloat16)
        if j == 0:
            pl.semaphore_wait(barrier, crew)

        @pl.when(owner)
        def cross():
            if j == 0:
                greet(near_sem, first + far[0])
            spread(far, j, PAIR if j == last else ALL, recv_sem.at[j])

            @pl.when(low)
            def tell():
                if j == 0:
                    for mate in mates:
                        greet(near_sem, mate + spot)

        @pl.when(jnp.logical_and(outer, low))
        def give_low():
            if j == 0:
                spread(near, j, ALL, recv_sem.at[j])
                pl.semaphore_wait(near_sem, 1)
                spread(far, j, ALL, recv_sem.at[j])
            elif j < last:
                spread(mixed, j, ALL, recv_sem.at[j])
            else:
                spread(mixed, j, ASK, asking())
                spread(mixed, j, PAIR, recv_sem.at[j])

        @pl.when(jnp.logical_and(outer, jnp.logical_not(low)))
        def give_high():
            spread(mixed, j, PAIR if j == last else ALL, recv_sem.at[j])
            if j == last:
                spread(mixed, j, ASK, asking())

    @pl.when(owner)
    def around():
        pl.semaphore_wait(near_sem, 1)
        for j in range(slots):
            spread(near[1:], j, PAIR if j == last else ALL, recv_sem.at[j])
            own(j, PAIR if j == last else ALL, recv_sem.at[j]).start()
        spread(near[1:], last, ASK, asking())
        own(last, ASK, asking()).start()

    def columns(j):
        return pl.ds(pl.multiple_of((j * owners + mine) * width, width), width)

    def back(j, other):
        return pltpu.make_async_remote_copy(
            src_ref=result.at[j, other],
            dst_ref=landed.at[:, columns(j)],
            send_sem=back_sem,
            recv_sem=home_sem,
            device_id={"sp": other},
            device_id_type=MESH,
        )

    def own_back(j):
        return pltpu.make_async_copy(result.at[j, me], landed.at[:, columns(j)], home_sem)

    factor = math.log2(math.e) / math.sqrt(width)

    def arrived(j):
        whole = held.at[j, :, PAIR] if j == last else held.at[j]
        pltpu.make_async_copy(whole, whole, recv_sem.at[j]).wait()

    def attend(j, chunk):
        picked = pl.ds(chunk * half, half)
        if j == last:
            asked = held.at[j, picked, ASK]
            pltpu.make_async_copy(asked, asked, query_sem.at[chunk]).wait()
        keys = held[j, :, 0].reshape(-1, width)
        values = held[j, :, 1].reshape(-1, width)
        queries = held[j, picked, 2].reshape(half * tokens, width)
        scores = lax.dot_general(
            queries, keys, (((1,), (1,)), ((), ())), preferred_element_type=jnp.float32
        )
        top = jnp.max(scores, axis=-1, keepdims=True)
        weights = jnp.exp2((scores - top) * factor)
        total = jnp.sum(weights, axis=-1, keepdims=True)
        attended = jnp.dot(
            weights.astype(jnp.bfloat16), values, preferred_element_type=jnp.float32
        ) / total
        result[j, picked] = attended.astype(jnp.bfloat16).reshape(half, tokens, width)

    def deliver(j, chunk, steps=None):
        for step in steps or range(half):
            back(j, chunk * half + step).start()

    def deliver_around(j, chunk):
        for step in range(half):
            other = chunk * half + step

            @pl.when(other != me)
            def give():
                back(j, other).start()

        own_back(j).start()

    inner = first // half
    opposite, beside = inner + 1 - side, inner + side
    head, tail = 0, chunks - 1

    def ask_across():
        spread(far, last, ASK, asking())

    def remaining():
        for start, stop in ((1, inner), (inner + 2, chunks - 1)):
            for j in range(slots if stop > start else 0):
                @pl.loop(start, stop)
                def step(chunk):
                    attend(j, chunk)
                    deliver(j, chunk)

    @pl.when(owner)
    def work():
        second = jnp.where(low, tail, opposite)
        third = jnp.where(low, opposite, tail)
        for j in range(slots):
            arrived(j)
            attend(j, head)
            deliver(j, head)
            if j == 0:
                ask_across()
            if j == 1:
                @pl.when(jnp.logical_not(low))
                def release_rest():
                    deliver(0, opposite, range(0, half))
            if j == last and last > 0:
                deliver(last - 1, second)
            attend(j, second)
            if j == 0:
                pl.when(low)(functools.partial(deliver, j, second))

                @pl.when(jnp.logical_not(low))
                def deliver_some():
                    pass
            elif j != last - 1:
                deliver(j, second)
            attend(j, third)
            deliver(j, third)
            attend(j, beside)
            deliver_around(j, beside)
        remaining()

        sent = send.at[:, pl.ds(0, owners - 1)]
        pltpu.make_async_copy(sent, sent, send_sem).wait()
        given = result.at[:, pl.ds(0, size - 1)]
        pltpu.make_async_copy(given, given, back_sem).wait()

    @pl.when(outer)
    def rest():
        pltpu.make_async_copy(send, send, send_sem).wait()

    pltpu.make_async_copy(landed, landed, home_sem).wait()


def shards(queries, keys, values):
    tokens, heads, width = queries.shape
    size = lax.axis_size("sp")
    owners = math.gcd(heads, size // 2)
    slots = heads // owners
    kind = queries.dtype
    return pl.pallas_call(
        functools.partial(kernel, owners, slots, size),
        out_shape=pltpu.VMEM((tokens, heads * width), kind),
        in_specs=[pl.BlockSpec(memory_space=pl.ANY)] * 3,
        out_specs=pl.BlockSpec(memory_space=pltpu.VMEM),
        scratch_shapes=[
            pltpu.VMEM((slots, 3, tokens, owners, width), kind),
            pltpu.VMEM((slots, 3, tokens * owners, width), jnp.float32),
            pltpu.VMEM((slots, owners, 3, tokens, width), kind),
            pltpu.VMEM((slots, size, 3, tokens, width), kind),
            pltpu.VMEM((slots, size, tokens, width), kind),
            pltpu.SemaphoreType.DMA((slots,)),
            pltpu.SemaphoreType.DMA,
            pltpu.SemaphoreType.DMA((slots,)),
            pltpu.SemaphoreType.DMA((2 * size // owners,)),
            pltpu.SemaphoreType.DMA,
            pltpu.SemaphoreType.DMA,
            pltpu.SemaphoreType.REGULAR,
        ],
        compiler_params=pltpu.CompilerParams(collective_id=0, has_side_effects=True),
    )(queries, keys, values)


def solution(mesh):
    return jax.shard_map(
        shards,
        mesh=mesh,
        in_specs=(
            P(("dp", "sp"), None, None),
            P(("dp", "sp"), None, None),
            P(("dp", "sp"), None, None),
        ),
        out_specs=P(("dp", "sp"), None),
        check_vma=False,
    )
```

```python
import functools
import math

import jax
import jax.numpy as jnp
from jax import lax
from jax.experimental import pallas as pl
from jax.experimental.pallas import tpu as pltpu
from jax.sharding import PartitionSpec as P

MESH = pl.DeviceIdType.MESH
ALL, PAIR, ASK = pl.ds(0, 3), pl.ds(0, 2), pl.ds(2, 1)


def kernel(
    owners, slots, size,
    q_hbm, k_hbm, v_hbm, landed,
    raw, wide, send, held, result,
    in_sem, send_sem, recv_sem, query_sem, back_sem, home_sem, near_sem,
):
    me = lax.axis_index("sp")
    tokens, _, width = q_hbm.shape
    first, half = (size - owners) // 2, owners // 2
    side = me // (size // 2)
    mine = me - first
    owner = jnp.logical_and(mine >= 0, mine < owners)
    outer = jnp.logical_not(owner)
    last = slots - 1
    chunks = size // half

    def load(j, i, src):
        return pltpu.make_async_copy(
            src.at[:, pl.ds(j * owners, owners), :], raw.at[j, i], in_sem.at[j]
        )

    for j in range(slots):
        for i, src in enumerate((k_hbm, v_hbm, q_hbm)):
            load(j, i, src).start()

    barrier = pltpu.get_barrier_semaphore()

    def greet(semaphore, other):
        pl.semaphore_signal(semaphore, inc=1, device_id={"sp": other}, device_id_type=MESH)

    spot = lax.rem(mine + size, half)
    far = [(1 - side) * half + lax.rem(spot + step, half) for step in range(half)]
    near = [side * half + lax.rem(spot + step, half) for step in range(half)]

    low = side == 0
    mates = range(0, first, half)

    @pl.when(owner)
    def enter():
        for to in far:
            greet(barrier, first + to)
        for other in range(first):
            greet(barrier, size - 1 - other)

        @pl.when(low)
        def enter_low():
            for other in range(first):
                greet(barrier, other)

    @pl.when(jnp.logical_and(outer, low))
    def enter_outer():
        greet(barrier, first + spot)

    def outward(j, to, parts, semaphore):
        return pltpu.make_async_remote_copy(
            src_ref=send.at[j, to, parts],
            dst_ref=held.at[j, me, parts],
            send_sem=send_sem,
            recv_sem=semaphore,
            device_id={"sp": first + to},
            device_id_type=MESH,
        )

    def own(j, parts, semaphore):
        return pltpu.make_async_copy(send.at[j, mine, parts], held.at[j, me, parts], semaphore)

    def asking():
        return query_sem.at[me // half]

    def spread(targets, j, parts, semaphore):
        for to in targets:
            outward(j, to, parts, semaphore).start()

    mixed = [to for pair in zip(far, near) for to in pair]
    crew = jnp.where(owner, half + jnp.where(low, len(mates), 0), jnp.where(low, half, owners))
    for j in range(slots):
        pltpu.make_async_copy(raw.at[j], raw.at[j], in_sem.at[j]).wait()
        for i in range(3):
            wide[j, i] = raw[j, i].astype(jnp.float32).reshape(tokens * owners, width)
        for to in range(owners):
            for i in range(3):
                rows = wide[j, i, pl.ds(to, tokens, stride=owners), :]
                send[j, to, i] = rows.astype(jnp.bfloat16)
        if j == 0:
            pl.semaphore_wait(barrier, crew)

        @pl.when(owner)
        def cross():
            if j == 0:
                greet(near_sem, first + far[0])
            spread(far, j, PAIR if j == last else ALL, recv_sem.at[j])

            @pl.when(low)
            def tell():
                if j == 0:
                    for mate in mates:
                        greet(near_sem, mate + spot)

        @pl.when(jnp.logical_and(outer, low))
        def give_low():
            if j == 0:
                spread(near, j, ALL, recv_sem.at[j])
                pl.semaphore_wait(near_sem, 1)
                spread(far, j, ALL, recv_sem.at[j])
            elif j < last:
                spread(mixed, j, ALL, recv_sem.at[j])
            else:
                spread(mixed, j, ASK, asking())
                spread(mixed, j, PAIR, recv_sem.at[j])

        @pl.when(jnp.logical_and(outer, jnp.logical_not(low)))
        def give_high():
            spread(mixed, j, PAIR if j == last else ALL, recv_sem.at[j])
            if j == last:
                spread(mixed, j, ASK, asking())

    @pl.when(owner)
    def around():
        pl.semaphore_wait(near_sem, 1)
        for j in range(slots):
            spread(near[1:], j, PAIR if j == last else ALL, recv_sem.at[j])
            own(j, PAIR if j == last else ALL, recv_sem.at[j]).start()
        spread(near[1:], last, ASK, asking())
        own(last, ASK, asking()).start()

    def columns(j):
        return pl.ds(pl.multiple_of((j * owners + mine) * width, width), width)

    def back(j, other):
        return pltpu.make_async_remote_copy(
            src_ref=result.at[j, other],
            dst_ref=landed.at[:, columns(j)],
            send_sem=back_sem,
            recv_sem=home_sem,
            device_id={"sp": other},
            device_id_type=MESH,
        )

    def own_back(j):
        return pltpu.make_async_copy(result.at[j, me], landed.at[:, columns(j)], home_sem)

    factor = math.log2(math.e) / math.sqrt(width)

    def arrived(j):
        whole = held.at[j, :, PAIR] if j == last else held.at[j]
        pltpu.make_async_copy(whole, whole, recv_sem.at[j]).wait()

    def attend(j, chunk, steps=None):
        steps = steps or range(half)
        if j == last and steps[0] == 0:
            asked = held.at[j, pl.ds(chunk * half, half), ASK]
            pltpu.make_async_copy(asked, asked, query_sem.at[chunk]).wait()
        picked = pl.ds(chunk * half + steps[0], len(steps))
        keys = held[j, :, 0].reshape(-1, width)
        values = held[j, :, 1].reshape(-1, width)
        queries = held[j, picked, 2].reshape(len(steps) * tokens, width)
        scores = lax.dot_general(
            queries, keys, (((1,), (1,)), ((), ())), preferred_element_type=jnp.float32
        )
        top = jnp.max(scores, axis=-1, keepdims=True)
        weights = jnp.exp2((scores - top) * factor)
        total = jnp.sum(weights, axis=-1, keepdims=True)
        attended = jnp.dot(
            weights.astype(jnp.bfloat16), values, preferred_element_type=jnp.float32
        ) / total
        result[j, picked] = attended.astype(jnp.bfloat16).reshape(len(steps), tokens, width)

    def deliver(j, chunk, steps=None):
        for step in steps or range(half):
            back(j, chunk * half + step).start()

    def deliver_around(j, chunk):
        for step in range(half):
            other = chunk * half + step

            @pl.when(other != me)
            def give():
                back(j, other).start()

        own_back(j).start()

    inner, wing = first // half, half // 2
    opposite, beside = inner + 1 - side, inner + side
    head, tail = 0, chunks - 1

    def ask_across():
        spread(far, last, ASK, asking())

    def remaining():
        for start, stop in ((1, inner), (inner + 2, chunks - 1)):
            for j in range(slots if stop > start else 0):
                @pl.loop(start, stop)
                def step(chunk):
                    attend(j, chunk)
                    deliver(j, chunk)

    @pl.when(owner)
    def work():
        second = jnp.where(low, tail, opposite)
        third = jnp.where(low, opposite, tail)
        high = jnp.logical_not(low)
        front, rear = range(wing), range(wing, half)
        for j in range(slots):
            arrived(j)
            for steps in (front, rear) if j == last else (range(half),):
                attend(j, head, steps)
                deliver(j, head, steps)
            if j == 0:
                pl.when(high)(ask_across)
            if j == 1:
                pl.when(high)(functools.partial(deliver, 0, opposite))
            if j == last:
                pl.when(low)(functools.partial(deliver, last - 1, tail))
                pl.when(high)(functools.partial(deliver, last - 1, opposite, front))
            attend(j, second)
            if j == last:
                deliver(j, second, front)
                pl.when(high)(functools.partial(deliver, last - 1, opposite, rear))
                deliver(j, second, rear)
            attend(j, third)
            if j == 0:
                pl.when(high)(functools.partial(deliver, j, tail))
            else:
                deliver(j, third)
            attend(j, beside)
            deliver_around(j, beside)
            if j == 0:
                @pl.when(low)
                def open_low():
                    ask_across()
                    deliver(0, tail)
                    deliver(0, opposite)
        remaining()

        sent = send.at[:, pl.ds(0, owners - 1)]
        pltpu.make_async_copy(sent, sent, send_sem).wait()
        given = result.at[:, pl.ds(0, size - 1)]
        pltpu.make_async_copy(given, given, back_sem).wait()

    @pl.when(outer)
    def rest():
        pltpu.make_async_copy(send, send, send_sem).wait()

    pltpu.make_async_copy(landed, landed, home_sem).wait()


def shards(queries, keys, values):
    tokens, heads, width = queries.shape
    size = lax.axis_size("sp")
    owners = math.gcd(heads, size // 2)
    slots = heads // owners
    kind = queries.dtype
    return pl.pallas_call(
        functools.partial(kernel, owners, slots, size),
        out_shape=pltpu.VMEM((tokens, heads * width), kind),
        in_specs=[pl.BlockSpec(memory_space=pl.ANY)] * 3,
        out_specs=pl.BlockSpec(memory_space=pltpu.VMEM),
        scratch_shapes=[
            pltpu.VMEM((slots, 3, tokens, owners, width), kind),
            pltpu.VMEM((slots, 3, tokens * owners, width), jnp.float32),
            pltpu.VMEM((slots, owners, 3, tokens, width), kind),
            pltpu.VMEM((slots, size, 3, tokens, width), kind),
            pltpu.VMEM((slots, size, tokens, width), kind),
            pltpu.SemaphoreType.DMA((slots,)),
            pltpu.SemaphoreType.DMA,
            pltpu.SemaphoreType.DMA((slots,)),
            pltpu.SemaphoreType.DMA((2 * size // owners,)),
            pltpu.SemaphoreType.DMA,
            pltpu.SemaphoreType.DMA,
            pltpu.SemaphoreType.REGULAR,
        ],
        compiler_params=pltpu.CompilerParams(collective_id=0, has_side_effects=True),
    )(queries, keys, values)


def solution(mesh):
    return jax.shard_map(
        shards,
        mesh=mesh,
        in_specs=(
            P(("dp", "sp"), None, None),
            P(("dp", "sp"), None, None),
            P(("dp", "sp"), None, None),
        ),
        out_specs=P(("dp", "sp"), None),
        check_vma=False,
    )
```

```python
import functools
import math

import jax
import jax.numpy as jnp
from jax import lax
from jax.experimental import pallas as pl
from jax.experimental.pallas import tpu as pltpu
from jax.sharding import PartitionSpec as P

MESH = pl.DeviceIdType.MESH
ALL, PAIR, ASK = pl.ds(0, 3), pl.ds(0, 2), pl.ds(2, 1)


def kernel(
    owners, slots, size,
    q_hbm, k_hbm, v_hbm, landed,
    raw, wide, send, held, result,
    in_sem, send_sem, recv_sem, query_sem, back_sem, home_sem, near_sem,
):
    me = lax.axis_index("sp")
    tokens, _, width = q_hbm.shape
    first, half = (size - owners) // 2, owners // 2
    side = me // (size // 2)
    mine = me - first
    owner = jnp.logical_and(mine >= 0, mine < owners)
    outer = jnp.logical_not(owner)
    last = slots - 1
    chunks = size // half

    def load(j, i, src):
        return pltpu.make_async_copy(
            src.at[:, pl.ds(j * owners, owners), :], raw.at[j, i], in_sem.at[j]
        )

    for j in range(slots):
        for i, src in enumerate((k_hbm, v_hbm, q_hbm)):
            load(j, i, src).start()

    barrier = pltpu.get_barrier_semaphore()

    def greet(semaphore, other):
        pl.semaphore_signal(semaphore, inc=1, device_id={"sp": other}, device_id_type=MESH)

    spot = lax.rem(mine + size, half)
    far = [(1 - side) * half + lax.rem(spot + step, half) for step in range(half)]
    near = [side * half + lax.rem(spot + step, half) for step in range(half)]

    low = side == 0
    mates = range(0, first, half)

    @pl.when(owner)
    def enter():
        for to in far:
            greet(barrier, first + to)
        for other in range(first):
            greet(barrier, size - 1 - other)

        @pl.when(low)
        def enter_low():
            for other in range(first):
                greet(barrier, other)

    @pl.when(jnp.logical_and(outer, low))
    def enter_outer():
        greet(barrier, first + spot)

    def outward(j, to, parts, semaphore):
        return pltpu.make_async_remote_copy(
            src_ref=send.at[j, to, parts],
            dst_ref=held.at[j, me, parts],
            send_sem=send_sem,
            recv_sem=semaphore,
            device_id={"sp": first + to},
            device_id_type=MESH,
        )

    def own(j, parts, semaphore):
        return pltpu.make_async_copy(send.at[j, mine, parts], held.at[j, me, parts], semaphore)

    def asking():
        return query_sem.at[me // half]

    def spread(targets, j, parts, semaphore):
        for to in targets:
            outward(j, to, parts, semaphore).start()

    mixed = [to for pair in zip(far, near) for to in pair]
    crew = jnp.where(owner, half + jnp.where(low, len(mates), 0), jnp.where(low, half, owners))
    for j in range(slots):
        pltpu.make_async_copy(raw.at[j], raw.at[j], in_sem.at[j]).wait()
        for i in range(3):
            wide[j, i] = raw[j, i].astype(jnp.float32).reshape(tokens * owners, width)
        for to in range(owners):
            for i in range(3):
                rows = wide[j, i, pl.ds(to, tokens, stride=owners), :]
                send[j, to, i] = rows.astype(jnp.bfloat16)
        if j == 0:
            pl.semaphore_wait(barrier, crew)

        @pl.when(owner)
        def cross():
            if j == 0:
                greet(near_sem, first + far[0])
            spread(far, j, PAIR if j == last else ALL, recv_sem.at[j])

            @pl.when(low)
            def tell():
                if j == 0:
                    for mate in mates:
                        greet(near_sem, mate + spot)

        @pl.when(jnp.logical_and(outer, low))
        def give_low():
            if j == 0:
                spread(near, j, ALL, recv_sem.at[j])
                pl.semaphore_wait(near_sem, 1)
                spread(far, j, ALL, recv_sem.at[j])
            elif j < last:
                spread(mixed, j, ALL, recv_sem.at[j])
            else:
                spread(mixed, j, ASK, asking())
                spread(mixed, j, PAIR, recv_sem.at[j])

        @pl.when(jnp.logical_and(outer, jnp.logical_not(low)))
        def give_high():
            spread(mixed, j, PAIR if j == last else ALL, recv_sem.at[j])
            if j == last:
                spread(mixed, j, ASK, asking())

    @pl.when(owner)
    def around():
        pl.semaphore_wait(near_sem, 1)
        for j in range(slots):
            spread(near[1:], j, PAIR if j == last else ALL, recv_sem.at[j])
            own(j, PAIR if j == last else ALL, recv_sem.at[j]).start()
        spread(near[1:], last, ASK, asking())
        own(last, ASK, asking()).start()

    def columns(j):
        return pl.ds(pl.multiple_of((j * owners + mine) * width, width), width)

    def back(j, other):
        return pltpu.make_async_remote_copy(
            src_ref=result.at[j, other],
            dst_ref=landed.at[:, columns(j)],
            send_sem=back_sem,
            recv_sem=home_sem,
            device_id={"sp": other},
            device_id_type=MESH,
        )

    def own_back(j):
        return pltpu.make_async_copy(result.at[j, me], landed.at[:, columns(j)], home_sem)

    factor = math.log2(math.e) / math.sqrt(width)

    def arrived(j):
        whole = held.at[j, :, PAIR] if j == last else held.at[j]
        pltpu.make_async_copy(whole, whole, recv_sem.at[j]).wait()

    def attend(j, chunk, steps=None):
        steps = steps or range(half)
        if j == last and steps[0] == 0:
            asked = held.at[j, pl.ds(chunk * half, half), ASK]
            pltpu.make_async_copy(asked, asked, query_sem.at[chunk]).wait()
        picked = pl.ds(chunk * half + steps[0], len(steps))
        keys = held[j, :, 0].reshape(-1, width)
        values = held[j, :, 1].reshape(-1, width)
        queries = held[j, picked, 2].reshape(len(steps) * tokens, width)
        scores = lax.dot_general(
            queries, keys, (((1,), (1,)), ((), ())), preferred_element_type=jnp.float32
        )
        top = jnp.max(scores, axis=-1, keepdims=True)
        weights = jnp.exp2((scores - top) * factor)
        total = jnp.sum(weights, axis=-1, keepdims=True)
        attended = jnp.dot(
            weights.astype(jnp.bfloat16), values, preferred_element_type=jnp.float32
        ) / total
        result[j, picked] = attended.astype(jnp.bfloat16).reshape(len(steps), tokens, width)

    def deliver(j, chunk, steps=None):
        for step in steps or range(half):
            step = step if chunk is head else step ^ 1
            back(j, chunk * half + step).start()

    def deliver_around(j, chunk):
        for step in range(half):
            other = chunk * half + step

            @pl.when(other != me)
            def give():
                back(j, other).start()

        own_back(j).start()

    inner, wing = first // half, half // 2
    opposite, beside = inner + 1 - side, inner + side
    head, tail = 0, chunks - 1

    def ask_across():
        spread(far, last, ASK, asking())

    def remaining():
        for start, stop in ((1, inner), (inner + 2, chunks - 1)):
            for j in range(slots if stop > start else 0):
                @pl.loop(start, stop)
                def step(chunk):
                    attend(j, chunk)
                    deliver(j, chunk)

    @pl.when(owner)
    def work():
        second = jnp.where(low, tail, opposite)
        third = jnp.where(low, opposite, tail)
        high = jnp.logical_not(low)
        front, rear = range(wing), range(wing, half)
        for j in range(slots):
            arrived(j)
            for steps in (front, rear) if j == last else (range(half),):
                attend(j, head, steps)
                deliver(j, head, steps)
            if j == 0:
                pl.when(high)(ask_across)
            if j == 1:
                pl.when(high)(functools.partial(deliver, 0, opposite))
            if j == last:
                pl.when(low)(functools.partial(deliver, last - 1, tail))
                pl.when(high)(functools.partial(deliver, last - 1, opposite, front))
            attend(j, second)
            if j == last:
                deliver(j, second, front)
                pl.when(high)(functools.partial(deliver, last - 1, opposite, rear))
                deliver(j, second, rear)
            attend(j, third)
            if j == 0:
                pl.when(high)(functools.partial(deliver, j, tail))
            else:
                deliver(j, third)
            attend(j, beside)
            deliver_around(j, beside)
            if j == 0:
                @pl.when(low)
                def open_low():
                    ask_across()
                    deliver(0, tail)
                    deliver(0, opposite)
        remaining()

        sent = send.at[:, pl.ds(0, owners - 1)]
        pltpu.make_async_copy(sent, sent, send_sem).wait()
        given = result.at[:, pl.ds(0, size - 1)]
        pltpu.make_async_copy(given, given, back_sem).wait()

    @pl.when(outer)
    def rest():
        pltpu.make_async_copy(send, send, send_sem).wait()

    pltpu.make_async_copy(landed, landed, home_sem).wait()


def shards(queries, keys, values):
    tokens, heads, width = queries.shape
    size = lax.axis_size("sp")
    owners = math.gcd(heads, size // 2)
    slots = heads // owners
    kind = queries.dtype
    return pl.pallas_call(
        functools.partial(kernel, owners, slots, size),
        out_shape=pltpu.VMEM((tokens, heads * width), kind),
        in_specs=[pl.BlockSpec(memory_space=pl.ANY)] * 3,
        out_specs=pl.BlockSpec(memory_space=pltpu.VMEM),
        scratch_shapes=[
            pltpu.VMEM((slots, 3, tokens, owners, width), kind),
            pltpu.VMEM((slots, 3, tokens * owners, width), jnp.float32),
            pltpu.VMEM((slots, owners, 3, tokens, width), kind),
            pltpu.VMEM((slots, size, 3, tokens, width), kind),
            pltpu.VMEM((slots, size, tokens, width), kind),
            pltpu.SemaphoreType.DMA((slots,)),
            pltpu.SemaphoreType.DMA,
            pltpu.SemaphoreType.DMA((slots,)),
            pltpu.SemaphoreType.DMA((2 * size // owners,)),
            pltpu.SemaphoreType.DMA,
            pltpu.SemaphoreType.DMA,
            pltpu.SemaphoreType.REGULAR,
        ],
        compiler_params=pltpu.CompilerParams(collective_id=0, has_side_effects=True),
    )(queries, keys, values)


def solution(mesh):
    return jax.shard_map(
        shards,
        mesh=mesh,
        in_specs=(
            P(("dp", "sp"), None, None),
            P(("dp", "sp"), None, None),
            P(("dp", "sp"), None, None),
        ),
        out_specs=P(("dp", "sp"), None),
        check_vma=False,
    )
```

```python
import functools
import math

import jax
import jax.numpy as jnp
from jax import lax
from jax.experimental import pallas as pl
from jax.experimental.pallas import tpu as pltpu
from jax.sharding import PartitionSpec as P

MESH = pl.DeviceIdType.MESH
ALL, PAIR, ASK = pl.ds(0, 3), pl.ds(0, 2), pl.ds(2, 1)


def kernel(
    owners, slots, size,
    q_hbm, k_hbm, v_hbm, landed,
    raw, wide, send, held, result,
    in_sem, send_sem, recv_sem, query_sem, back_sem, home_sem, near_sem,
):
    me = lax.axis_index("sp")
    tokens, _, width = q_hbm.shape
    first, half = (size - owners) // 2, owners // 2
    side = me // (size // 2)
    mine = me - first
    owner = jnp.logical_and(mine >= 0, mine < owners)
    outer = jnp.logical_not(owner)
    last = slots - 1
    chunks = size // half

    def load(j, i, src):
        return pltpu.make_async_copy(
            src.at[:, pl.ds(j * owners, owners), :], raw.at[j, i], in_sem.at[j]
        )

    for j in range(slots):
        for i, src in enumerate((k_hbm, v_hbm, q_hbm)):
            load(j, i, src).start()

    barrier = pltpu.get_barrier_semaphore()

    def greet(semaphore, other):
        pl.semaphore_signal(semaphore, inc=1, device_id={"sp": other}, device_id_type=MESH)

    spot = lax.rem(mine + size, half)
    far = [(1 - side) * half + lax.rem(spot + step, half) for step in range(half)]
    near = [side * half + lax.rem(spot + step, half) for step in range(half)]

    low = side == 0
    mates = range(0, first, half)

    @pl.when(owner)
    def enter():
        for to in far:
            greet(barrier, first + to)
        for other in range(first):
            greet(barrier, size - 1 - other)

        @pl.when(low)
        def enter_low():
            for other in range(first):
                greet(barrier, other)

    @pl.when(jnp.logical_and(outer, low))
    def enter_outer():
        greet(barrier, first + spot)

    def outward(j, to, parts, semaphore):
        return pltpu.make_async_remote_copy(
            src_ref=send.at[j, to, parts],
            dst_ref=held.at[j, me, parts],
            send_sem=send_sem,
            recv_sem=semaphore,
            device_id={"sp": first + to},
            device_id_type=MESH,
        )

    def landing(j):
        return recv_sem.at[jnp.where(me < half, slots, last) if j == last else j]

    def own(j, parts, semaphore):
        return pltpu.make_async_copy(send.at[j, mine, parts], held.at[j, me, parts], semaphore)

    def asking():
        return query_sem.at[me // half]

    def spread(targets, j, parts, semaphore):
        for to in targets:
            outward(j, to, parts, semaphore).start()

    mixed = [to for pair in zip(far, near) for to in pair]
    crew = jnp.where(owner, half + jnp.where(low, len(mates), 0), jnp.where(low, half, owners))
    for j in range(slots):
        pltpu.make_async_copy(raw.at[j], raw.at[j], in_sem.at[j]).wait()
        for i in range(3):
            wide[j, i] = raw[j, i].astype(jnp.float32).reshape(tokens * owners, width)
        for to in range(owners):
            for i in range(3):
                rows = wide[j, i, pl.ds(to, tokens, stride=owners), :]
                send[j, to, i] = rows.astype(jnp.bfloat16)
        if j == 0:
            pl.semaphore_wait(barrier, crew)

        @pl.when(owner)
        def cross():
            if j == 0:
                greet(near_sem, first + far[0])
            spread(far, j, PAIR if j == last else ALL, landing(j))

            @pl.when(low)
            def tell():
                if j == 0:
                    for mate in mates:
                        greet(near_sem, mate + spot)

        @pl.when(jnp.logical_and(outer, low))
        def give_low():
            if j == 0:
                spread(near, j, ALL, recv_sem.at[j])
                pl.semaphore_wait(near_sem, 1)
                spread(far, j, ALL, recv_sem.at[j])
            elif j < last:
                spread(mixed, j, ALL, recv_sem.at[j])
            else:
                spread(mixed, j, ASK, asking())
                spread(mixed, j, PAIR, landing(j))

        @pl.when(jnp.logical_and(outer, jnp.logical_not(low)))
        def give_high():
            spread(mixed, j, PAIR if j == last else ALL, landing(j))
            if j == last:
                spread(mixed, j, ASK, asking())

    @pl.when(owner)
    def around():
        pl.semaphore_wait(near_sem, 1)
        for j in range(slots):
            spread(near[1:], j, PAIR if j == last else ALL, landing(j))
            own(j, PAIR if j == last else ALL, landing(j)).start()
        spread(near[1:], last, ASK, asking())
        own(last, ASK, asking()).start()

    def columns(j):
        return pl.ds(pl.multiple_of((j * owners + mine) * width, width), width)

    def back(j, other):
        return pltpu.make_async_remote_copy(
            src_ref=result.at[j, other],
            dst_ref=landed.at[:, columns(j)],
            send_sem=back_sem,
            recv_sem=home_sem,
            device_id={"sp": other},
            device_id_type=MESH,
        )

    def own_back(j):
        return pltpu.make_async_copy(result.at[j, me], landed.at[:, columns(j)], home_sem)

    factor = math.log2(math.e) / math.sqrt(width)

    def arrived(j):
        whole = held.at[j, pl.ds(half, size - half), PAIR] if j == last else held.at[j]
        pltpu.make_async_copy(whole, whole, recv_sem.at[j]).wait()

    def product(queries, keys):
        return lax.dot_general(
            queries, keys, (((1,), (1,)), ((), ())), preferred_element_type=jnp.float32
        )

    def attend_split(j, chunk):
        asked = held.at[j, pl.ds(chunk * half, half), ASK]
        pltpu.make_async_copy(asked, asked, query_sem.at[chunk]).wait()
        queries = held[j, pl.ds(chunk * half, half), 2].reshape(half * tokens, width)
        scores = product(queries, held[j, pl.ds(half, size - half), 0].reshape(-1, width))
        early = jnp.max(scores, axis=-1, keepdims=True)
        weights = jnp.exp2((scores - early) * factor)
        total = jnp.sum(weights, axis=-1, keepdims=True)
        values = held[j, pl.ds(half, size - half), 1].reshape(-1, width)
        attended = jnp.dot(weights.astype(jnp.bfloat16), values, preferred_element_type=jnp.float32)

        rest = held.at[j, pl.ds(0, half), PAIR]
        pltpu.make_async_copy(rest, rest, recv_sem.at[slots]).wait()
        scores = product(queries, held[j, pl.ds(0, half), 0].reshape(-1, width))
        top = jnp.maximum(early, jnp.max(scores, axis=-1, keepdims=True))
        weights = jnp.exp2((scores - top) * factor)
        scale = jnp.exp2((early - top) * factor)
        total = total * scale + jnp.sum(weights, axis=-1, keepdims=True)
        values = held[j, pl.ds(0, half), 1].reshape(-1, width)
        attended = attended * scale + jnp.dot(
            weights.astype(jnp.bfloat16), values, preferred_element_type=jnp.float32
        )
        result[j, pl.ds(chunk * half, half)] = (
            (attended / total).astype(jnp.bfloat16).reshape(half, tokens, width)
        )

    def attend(j, chunk):
        picked = pl.ds(chunk * half, half)
        if j == last:
            asked = held.at[j, picked, ASK]
            pltpu.make_async_copy(asked, asked, query_sem.at[chunk]).wait()
        keys = held[j, :, 0].reshape(-1, width)
        values = held[j, :, 1].reshape(-1, width)
        queries = held[j, picked, 2].reshape(half * tokens, width)
        scores = lax.dot_general(
            queries, keys, (((1,), (1,)), ((), ())), preferred_element_type=jnp.float32
        )
        top = jnp.max(scores, axis=-1, keepdims=True)
        weights = jnp.exp2((scores - top) * factor)
        total = jnp.sum(weights, axis=-1, keepdims=True)
        attended = jnp.dot(
            weights.astype(jnp.bfloat16), values, preferred_element_type=jnp.float32
        ) / total
        result[j, picked] = attended.astype(jnp.bfloat16).reshape(half, tokens, width)

    def deliver(j, chunk, steps=None):
        for step in steps or range(half):
            step = step if chunk is head else step ^ 1
            back(j, chunk * half + step).start()

    def deliver_around(j, chunk):
        for step in range(half):
            other = chunk * half + step

            @pl.when(other != me)
            def give():
                back(j, other).start()

        own_back(j).start()

    inner, wing = first // half, half // 2
    opposite, beside = inner + 1 - side, inner + side
    head, tail = 0, chunks - 1

    def ask_across():
        spread(far, last, ASK, asking())

    def remaining():
        for start, stop in ((1, inner), (inner + 2, chunks - 1)):
            for j in range(slots if stop > start else 0):
                @pl.loop(start, stop)
                def step(chunk):
                    attend(j, chunk)
                    deliver(j, chunk)

    @pl.when(owner)
    def work():
        second = jnp.where(low, tail, opposite)
        third = jnp.where(low, opposite, tail)
        high = jnp.logical_not(low)
        front, rear = range(wing), range(wing, half)
        for j in range(slots):
            arrived(j)
            (attend_split if j == last else attend)(j, head)
            deliver(j, head)
            if j == 0:
                pl.when(high)(ask_across)
            if j == 1:
                pl.when(high)(functools.partial(deliver, 0, opposite))
            if j == last:
                pl.when(low)(functools.partial(deliver, last - 1, tail))
                pl.when(high)(functools.partial(deliver, last - 1, opposite, front))
            attend(j, second)
            if j == last:
                deliver(j, second, front)
                pl.when(high)(functools.partial(deliver, last - 1, opposite, rear))
                deliver(j, second, rear)
            attend(j, third)
            if j == 0:
                pl.when(high)(functools.partial(deliver, j, tail))
            else:
                deliver(j, third)
            attend(j, beside)
            deliver_around(j, beside)
            if j == 0:
                @pl.when(low)
                def open_low():
                    ask_across()
                    deliver(0, tail)
                    deliver(0, opposite)
        remaining()

        sent = send.at[:, pl.ds(0, owners - 1)]
        pltpu.make_async_copy(sent, sent, send_sem).wait()
        given = result.at[:, pl.ds(0, size - 1)]
        pltpu.make_async_copy(given, given, back_sem).wait()

    @pl.when(outer)
    def rest():
        pltpu.make_async_copy(send, send, send_sem).wait()

    pltpu.make_async_copy(landed, landed, home_sem).wait()


def shards(queries, keys, values):
    tokens, heads, width = queries.shape
    size = lax.axis_size("sp")
    owners = math.gcd(heads, size // 2)
    slots = heads // owners
    kind = queries.dtype
    return pl.pallas_call(
        functools.partial(kernel, owners, slots, size),
        out_shape=pltpu.VMEM((tokens, heads * width), kind),
        in_specs=[pl.BlockSpec(memory_space=pl.ANY)] * 3,
        out_specs=pl.BlockSpec(memory_space=pltpu.VMEM),
        scratch_shapes=[
            pltpu.VMEM((slots, 3, tokens, owners, width), kind),
            pltpu.VMEM((slots, 3, tokens * owners, width), jnp.float32),
            pltpu.VMEM((slots, owners, 3, tokens, width), kind),
            pltpu.VMEM((slots, size, 3, tokens, width), kind),
            pltpu.VMEM((slots, size, tokens, width), kind),
            pltpu.SemaphoreType.DMA((slots,)),
            pltpu.SemaphoreType.DMA,
            pltpu.SemaphoreType.DMA((slots + 1,)),
            pltpu.SemaphoreType.DMA((2 * size // owners,)),
            pltpu.SemaphoreType.DMA,
            pltpu.SemaphoreType.DMA,
            pltpu.SemaphoreType.REGULAR,
        ],
        compiler_params=pltpu.CompilerParams(collective_id=0, has_side_effects=True),
    )(queries, keys, values)


def solution(mesh):
    return jax.shard_map(
        shards,
        mesh=mesh,
        in_specs=(
            P(("dp", "sp"), None, None),
            P(("dp", "sp"), None, None),
            P(("dp", "sp"), None, None),
        ),
        out_specs=P(("dp", "sp"), None),
        check_vma=False,
    )
```

```python
import functools
import math

import jax
import jax.numpy as jnp
from jax import lax
from jax.experimental import pallas as pl
from jax.experimental.pallas import tpu as pltpu
from jax.sharding import PartitionSpec as P

MESH = pl.DeviceIdType.MESH
ALL, PAIR, ASK = pl.ds(0, 3), pl.ds(0, 2), pl.ds(2, 1)


def kernel(
    owners, slots, size,
    q_hbm, k_hbm, v_hbm, landed,
    raw, wide, send, held, result,
    in_sem, send_sem, recv_sem, query_sem, back_sem, home_sem, near_sem, cross_sem,
):
    me = lax.axis_index("sp")
    tokens, _, width = q_hbm.shape
    first, half = (size - owners) // 2, owners // 2
    side = me // (size // 2)
    mine = me - first
    owner = jnp.logical_and(mine >= 0, mine < owners)
    outer = jnp.logical_not(owner)
    last = slots - 1
    chunks = size // half

    def load(j, i, src):
        return pltpu.make_async_copy(
            src.at[:, pl.ds(j * owners, owners), :], raw.at[j, i], in_sem.at[j]
        )

    for j in range(slots):
        for i, src in enumerate((k_hbm, v_hbm, q_hbm)):
            load(j, i, src).start()

    barrier = pltpu.get_barrier_semaphore()

    def greet(semaphore, other):
        pl.semaphore_signal(semaphore, inc=1, device_id={"sp": other}, device_id_type=MESH)

    spot = lax.rem(mine + size, half)
    far = [(1 - side) * half + lax.rem(spot + step, half) for step in range(half)]
    near = [side * half + lax.rem(spot + step, half) for step in range(half)]

    low = side == 0
    mates = range(0, first, half)

    wing = half // 2
    lead = jnp.logical_and(spot < wing, side > 0)
    lower = [(1 - side) * half + lax.rem(spot + step, wing) for step in range(wing)]
    upper = [to + wing for to in lower]
    beyond = first + side * half + lax.rem(spot + wing, half)

    @pl.when(owner)
    def enter():
        for to in upper:
            greet(barrier, first + to)

        @pl.when(jnp.logical_or(spot < wing, side > 0))
        def enter_lower():
            for to in lower:
                greet(barrier, first + to)

        @pl.when(lead)
        def enter_lead():
            greet(barrier, beyond)

        for other in range(first):
            greet(barrier, size - 1 - other)

        @pl.when(low)
        def enter_low():
            for other in range(first):
                greet(barrier, other)

    @pl.when(jnp.logical_and(outer, low))
    def enter_outer():
        greet(barrier, first + spot)

    def outward(j, to, parts, semaphore):
        return pltpu.make_async_remote_copy(
            src_ref=send.at[j, to, parts],
            dst_ref=held.at[j, me, parts],
            send_sem=send_sem,
            recv_sem=semaphore,
            device_id={"sp": first + to},
            device_id_type=MESH,
        )

    def own(j, parts, semaphore):
        return pltpu.make_async_copy(send.at[j, mine, parts], held.at[j, me, parts], semaphore)

    def asking():
        return query_sem.at[me // half]

    def spread(targets, j, parts, semaphore):
        for to in targets:
            outward(j, to, parts, semaphore).start()

    mixed = [to for pair in zip(far, near) for to in pair]
    crew = jnp.where(owner, jnp.where(lead, wing, half) + jnp.where(low, len(mates), jnp.where(lead, 0, 1)), jnp.where(low, half, owners))
    for j in range(slots):
        pltpu.make_async_copy(raw.at[j], raw.at[j], in_sem.at[j]).wait()
        for i in range(3):
            wide[j, i] = raw[j, i].astype(jnp.float32).reshape(tokens * owners, width)
        for to in range(owners):
            for i in range(3):
                rows = wide[j, i, pl.ds(to, tokens, stride=owners), :]
                send[j, to, i] = rows.astype(jnp.bfloat16)
        if j == 0:
            pl.semaphore_wait(barrier, crew)

        @pl.when(owner)
        def cross():
            def tell():
                greet(near_sem, first + far[0])

                @pl.when(low)
                def tell_mates():
                    for mate in mates:
                        greet(near_sem, mate + spot)

            if j == 0:
                @pl.when(lead)
                def start_lead():
                    spread(lower, 0, ALL, recv_sem.at[0])

                @pl.when(jnp.logical_not(lead))
                def start_rest():
                    pl.when(jnp.logical_not(low))(functools.partial(greet, cross_sem, beyond))
                    tell()
                    spread(far, 0, ALL, recv_sem.at[0])

            if j == 1:
                @pl.when(lead)
                def follow():
                    pl.semaphore_wait(cross_sem, 1)
                    tell()
                    spread(upper, 0, ALL, recv_sem.at[0])

            if j > 0:
                spread(far, j, PAIR if j == last else ALL, recv_sem.at[j])

        @pl.when(jnp.logical_and(outer, low))
        def give_low():
            if j == 0:
                spread(near, j, ALL, recv_sem.at[j])
                pl.semaphore_wait(near_sem, 1)
                spread(far, j, ALL, recv_sem.at[j])
            elif j < last:
                spread(mixed, j, ALL, recv_sem.at[j])
            else:
                spread(mixed, j, ASK, asking())
                spread(mixed, j, PAIR, recv_sem.at[j])

        @pl.when(jnp.logical_and(outer, jnp.logical_not(low)))
        def give_high():
            spread(mixed, j, PAIR if j == last else ALL, recv_sem.at[j])
            if j == last:
                spread(mixed, j, ASK, asking())

    @pl.when(owner)
    def around():
        pl.semaphore_wait(near_sem, 1)
        for j in range(slots):
            spread(near[1:], j, PAIR if j == last else ALL, recv_sem.at[j])
            own(j, PAIR if j == last else ALL, recv_sem.at[j]).start()
        spread(near[1:], last, ASK, asking())
        own(last, ASK, asking()).start()

    def columns(j):
        return pl.ds(pl.multiple_of((j * owners + mine) * width, width), width)

    def back(j, other):
        return pltpu.make_async_remote_copy(
            src_ref=result.at[j, other],
            dst_ref=landed.at[:, columns(j)],
            send_sem=back_sem,
            recv_sem=home_sem,
            device_id={"sp": other},
            device_id_type=MESH,
        )

    def own_back(j):
        return pltpu.make_async_copy(result.at[j, me], landed.at[:, columns(j)], home_sem)

    factor = math.log2(math.e) / math.sqrt(width)

    def arrived(j):
        whole = held.at[j, :, PAIR] if j == last else held.at[j]
        pltpu.make_async_copy(whole, whole, recv_sem.at[j]).wait()

    def attend(j, chunk, steps=None):
        steps = steps or range(half)
        if j == last and steps[0] == 0:
            asked = held.at[j, pl.ds(chunk * half, half), ASK]
            pltpu.make_async_copy(asked, asked, query_sem.at[chunk]).wait()
        picked = pl.ds(chunk * half + steps[0], len(steps))
        keys = held[j, :, 0].reshape(-1, width)
        values = held[j, :, 1].reshape(-1, width)
        queries = held[j, picked, 2].reshape(len(steps) * tokens, width)
        scores = lax.dot_general(
            queries, keys, (((1,), (1,)), ((), ())), preferred_element_type=jnp.float32
        )
        top = jnp.max(scores, axis=-1, keepdims=True)
        weights = jnp.exp2((scores - top) * factor)
        total = jnp.sum(weights, axis=-1, keepdims=True)
        attended = jnp.dot(
            weights.astype(jnp.bfloat16), values, preferred_element_type=jnp.float32
        ) / total
        result[j, picked] = attended.astype(jnp.bfloat16).reshape(len(steps), tokens, width)

    def deliver(j, chunk, steps=None):
        for step in steps or range(half):
            step = step if chunk is head else step ^ 1
            back(j, chunk * half + step).start()

    def deliver_around(j, chunk):
        for step in range(half):
            other = chunk * half + step

            @pl.when(other != me)
            def give():
                back(j, other).start()

        own_back(j).start()

    inner = first // half
    opposite, beside = inner + 1 - side, inner + side
    head, tail = 0, chunks - 1

    def ask_across():
        spread(far, last, ASK, asking())

    def remaining():
        for start, stop in ((1, inner), (inner + 2, chunks - 1)):
            for j in range(slots if stop > start else 0):
                @pl.loop(start, stop)
                def step(chunk):
                    attend(j, chunk)
                    deliver(j, chunk)

    @pl.when(owner)
    def work():
        second = jnp.where(low, tail, opposite)
        third = jnp.where(low, opposite, tail)
        high = jnp.logical_not(low)
        front, rear = range(wing), range(wing, half)
        for j in range(slots):
            arrived(j)
            for steps in (front, rear) if j == last else (range(half),):
                attend(j, head, steps)
                deliver(j, head, steps)
            if j == 0:
                pl.when(high)(ask_across)
            if j == 1:
                pl.when(high)(functools.partial(deliver, 0, opposite))
            if j == last:
                pl.when(low)(functools.partial(deliver, last - 1, tail))
                pl.when(high)(functools.partial(deliver, last - 1, opposite, front))
            attend(j, second)
            if j == last:
                deliver(j, second, front)
                pl.when(high)(functools.partial(deliver, last - 1, opposite, rear))
                deliver(j, second, rear)
            attend(j, third)
            if j == 0:
                pl.when(high)(functools.partial(deliver, j, tail))
            else:
                deliver(j, third)
            attend(j, beside)
            deliver_around(j, beside)
            if j == 0:
                @pl.when(low)
                def open_low():
                    ask_across()
                    deliver(0, tail)
                    deliver(0, opposite)
        remaining()

        sent = send.at[:, pl.ds(0, owners - 1)]
        pltpu.make_async_copy(sent, sent, send_sem).wait()
        given = result.at[:, pl.ds(0, size - 1)]
        pltpu.make_async_copy(given, given, back_sem).wait()

    @pl.when(outer)
    def rest():
        pltpu.make_async_copy(send, send, send_sem).wait()

    pltpu.make_async_copy(landed, landed, home_sem).wait()


def shards(queries, keys, values):
    tokens, heads, width = queries.shape
    size = lax.axis_size("sp")
    owners = math.gcd(heads, size // 2)
    slots = heads // owners
    kind = queries.dtype
    return pl.pallas_call(
        functools.partial(kernel, owners, slots, size),
        out_shape=pltpu.VMEM((tokens, heads * width), kind),
        in_specs=[pl.BlockSpec(memory_space=pl.ANY)] * 3,
        out_specs=pl.BlockSpec(memory_space=pltpu.VMEM),
        scratch_shapes=[
            pltpu.VMEM((slots, 3, tokens, owners, width), kind),
            pltpu.VMEM((slots, 3, tokens * owners, width), jnp.float32),
            pltpu.VMEM((slots, owners, 3, tokens, width), kind),
            pltpu.VMEM((slots, size, 3, tokens, width), kind),
            pltpu.VMEM((slots, size, tokens, width), kind),
            pltpu.SemaphoreType.DMA((slots,)),
            pltpu.SemaphoreType.DMA,
            pltpu.SemaphoreType.DMA((slots,)),
            pltpu.SemaphoreType.DMA((2 * size // owners,)),
            pltpu.SemaphoreType.DMA,
            pltpu.SemaphoreType.DMA,
            pltpu.SemaphoreType.REGULAR,
            pltpu.SemaphoreType.REGULAR,
        ],
        compiler_params=pltpu.CompilerParams(collective_id=0, has_side_effects=True),
    )(queries, keys, values)


def solution(mesh):
    return jax.shard_map(
        shards,
        mesh=mesh,
        in_specs=(
            P(("dp", "sp"), None, None),
            P(("dp", "sp"), None, None),
            P(("dp", "sp"), None, None),
        ),
        out_specs=P(("dp", "sp"), None),
        check_vma=False,
    )
```

```python
import functools
import math

import jax
import jax.numpy as jnp
from jax import lax
from jax.experimental import pallas as pl
from jax.experimental.pallas import tpu as pltpu
from jax.sharding import PartitionSpec as P

MESH = pl.DeviceIdType.MESH
ALL, PAIR, ASK = pl.ds(0, 3), pl.ds(0, 2), pl.ds(2, 1)


def kernel(
    owners, slots, size,
    q_hbm, k_hbm, v_hbm, landed,
    raw, wide, send, held, result,
    in_sem, send_sem, recv_sem, query_sem, back_sem, home_sem, near_sem,
):
    me = lax.axis_index("sp")
    tokens, _, width = q_hbm.shape
    first, half = (size - owners) // 2, owners // 2
    side = me // (size // 2)
    mine = me - first
    owner = jnp.logical_and(mine >= 0, mine < owners)
    outer = jnp.logical_not(owner)
    last = slots - 1
    chunks = size // half

    def load(j, i, src):
        return pltpu.make_async_copy(
            src.at[:, pl.ds(j * owners, owners), :], raw.at[j, i], in_sem.at[j]
        )

    for j in range(slots):
        for i, src in enumerate((k_hbm, v_hbm, q_hbm)):
            load(j, i, src).start()

    barrier = pltpu.get_barrier_semaphore()

    def greet(semaphore, other):
        pl.semaphore_signal(semaphore, inc=1, device_id={"sp": other}, device_id_type=MESH)

    spot = lax.rem(mine + size, half)
    far = [(1 - side) * half + lax.rem(spot + step, half) for step in range(half)]
    near = [side * half + lax.rem(spot + step, half) for step in range(half)]

    low = side == 0
    mates = range(0, first, half)

    @pl.when(owner)
    def enter():
        for to in far:
            greet(barrier, first + to)
        for other in range(first):
            greet(barrier, size - 1 - other)

        @pl.when(low)
        def enter_low():
            for other in range(first):
                greet(barrier, other)

    @pl.when(jnp.logical_and(outer, low))
    def enter_outer():
        greet(barrier, first + spot)

    def outward(j, to, parts, semaphore):
        return pltpu.make_async_remote_copy(
            src_ref=send.at[j, to, parts],
            dst_ref=held.at[j, me, parts],
            send_sem=send_sem,
            recv_sem=semaphore,
            device_id={"sp": first + to},
            device_id_type=MESH,
        )

    def own(j, parts, semaphore):
        return pltpu.make_async_copy(send.at[j, mine, parts], held.at[j, me, parts], semaphore)

    def asking():
        return query_sem.at[me // half]

    def spread(targets, j, parts, semaphore):
        for to in targets:
            outward(j, to, parts, semaphore).start()

    mixed = [to for pair in zip(far, near) for to in pair]
    crew = jnp.where(owner, half + jnp.where(low, len(mates), 0), jnp.where(low, half, owners))
    for j in range(slots):
        pltpu.make_async_copy(raw.at[j], raw.at[j], in_sem.at[j]).wait()
        for i in range(3):
            wide[j, i] = raw[j, i].astype(jnp.float32).reshape(tokens * owners, width)
        for to in range(owners):
            for i in range(3):
                rows = wide[j, i, pl.ds(to, tokens, stride=owners), :]
                send[j, to, i] = rows.astype(jnp.bfloat16)
        if j == 0:
            pl.semaphore_wait(barrier, crew)

        @pl.when(owner)
        def cross():
            if j == 0:
                greet(near_sem, first + far[0])
            spread(far, j, PAIR if j == last else ALL, recv_sem.at[j])

            @pl.when(low)
            def tell():
                if j == 0:
                    for mate in mates:
                        greet(near_sem, mate + spot)

        @pl.when(jnp.logical_and(outer, low))
        def give_low():
            if j == 0:
                spread(near, j, ALL, recv_sem.at[j])
                pl.semaphore_wait(near_sem, 1)
                spread(far, j, ALL, recv_sem.at[j])
            elif j < last:
                spread(mixed, j, ALL, recv_sem.at[j])
            else:
                spread(mixed, j, ASK, asking())
                spread(mixed, j, PAIR, recv_sem.at[j])

        @pl.when(jnp.logical_and(outer, jnp.logical_not(low)))
        def give_high():
            spread(mixed, j, PAIR if j == last else ALL, recv_sem.at[j])
            if j == last:
                spread(mixed, j, ASK, asking())

    @pl.when(owner)
    def around():
        pl.semaphore_wait(near_sem, 1)
        for j in range(slots):
            spread(near[1:], j, PAIR if j == last else ALL, recv_sem.at[j])
            own(j, PAIR if j == last else ALL, recv_sem.at[j]).start()
        spread(near[1:], last, ASK, asking())
        own(last, ASK, asking()).start()

    def columns(j):
        return pl.ds(pl.multiple_of((j * owners + mine) * width, width), width)

    def back(j, other):
        return pltpu.make_async_remote_copy(
            src_ref=result.at[j, other],
            dst_ref=landed.at[:, columns(j)],
            send_sem=back_sem,
            recv_sem=home_sem,
            device_id={"sp": other},
            device_id_type=MESH,
        )

    def own_back(j):
        return pltpu.make_async_copy(result.at[j, me], landed.at[:, columns(j)], home_sem)

    factor = math.log2(math.e) / math.sqrt(width)

    def arrived(j):
        whole = held.at[j, :, PAIR] if j == last else held.at[j]
        pltpu.make_async_copy(whole, whole, recv_sem.at[j]).wait()

    def attend(j, chunk, steps=None):
        steps = steps or range(half)
        if j == last and steps[0] == 0:
            asked = held.at[j, pl.ds(chunk * half, half), ASK]
            pltpu.make_async_copy(asked, asked, query_sem.at[chunk]).wait()
        picked = pl.ds(chunk * half + steps[0], len(steps))
        keys = held[j, :, 0].reshape(-1, width)
        values = held[j, :, 1].reshape(-1, width)
        queries = held[j, picked, 2].reshape(len(steps) * tokens, width)
        scores = lax.dot_general(
            queries, keys, (((1,), (1,)), ((), ())), preferred_element_type=jnp.float32
        )
        top = jnp.max(scores, axis=-1, keepdims=True)
        weights = jnp.exp2((scores - top) * factor)
        total = jnp.sum(weights, axis=-1, keepdims=True)
        attended = jnp.dot(
            weights.astype(jnp.bfloat16), values, preferred_element_type=jnp.float32
        ) / total
        result[j, picked] = attended.astype(jnp.bfloat16).reshape(len(steps), tokens, width)

    def deliver(j, chunk, steps=None):
        for step in steps or range(half):
            step = step if chunk is head else step ^ 1
            back(j, chunk * half + step).start()

    def deliver_around(j, chunk):
        for step in range(half):
            other = chunk * half + step

            @pl.when(other != me)
            def give():
                back(j, other).start()

        own_back(j).start()

    inner, wing = first // half, half // 2
    opposite, beside = inner + 1 - side, inner + side
    head, tail = 0, chunks - 1

    def ask_across():
        spread(far, last, ASK, asking())

    def remaining():
        for start, stop in ((1, inner), (inner + 2, chunks - 1)):
            for j in range(slots if stop > start else 0):
                @pl.loop(start, stop)
                def step(chunk):
                    attend(j, chunk)
                    deliver(j, chunk)

    @pl.when(owner)
    def work():
        second = jnp.where(low, tail, opposite)
        third = jnp.where(low, opposite, tail)
        high = jnp.logical_not(low)
        front, rear = range(wing), range(wing, half)
        for j in range(slots):
            arrived(j)
            for steps in (front, rear) if j == last else (range(half),):
                attend(j, head, steps)
                deliver(j, head, steps)
            if j == 0:
                pl.when(high)(ask_across)
            if j == 1:
                pl.when(high)(functools.partial(deliver, 0, opposite, range(half - 1)))
            if j == last:
                pl.when(low)(functools.partial(deliver, last - 1, tail))
                pl.when(high)(functools.partial(deliver, 0, opposite, range(half - 1, half)))
                pl.when(high)(functools.partial(deliver, last - 1, opposite, front))
            attend(j, second)
            if j == last:
                deliver(j, second, front)
                pl.when(high)(functools.partial(deliver, last - 1, opposite, rear))
                deliver(j, second, rear)
            attend(j, third)
            if j == 0:
                pl.when(high)(functools.partial(deliver, j, tail))
            else:
                deliver(j, third)
            attend(j, beside)
            deliver_around(j, beside)
            if j == 0:
                @pl.when(low)
                def open_low():
                    ask_across()
                    deliver(0, tail)
                    deliver(0, opposite)
        remaining()

        sent = send.at[:, pl.ds(0, owners - 1)]
        pltpu.make_async_copy(sent, sent, send_sem).wait()
        given = result.at[:, pl.ds(0, size - 1)]
        pltpu.make_async_copy(given, given, back_sem).wait()

    @pl.when(outer)
    def rest():
        pltpu.make_async_copy(send, send, send_sem).wait()

    pltpu.make_async_copy(landed, landed, home_sem).wait()


def shards(queries, keys, values):
    tokens, heads, width = queries.shape
    size = lax.axis_size("sp")
    owners = math.gcd(heads, size // 2)
    slots = heads // owners
    kind = queries.dtype
    return pl.pallas_call(
        functools.partial(kernel, owners, slots, size),
        out_shape=pltpu.VMEM((tokens, heads * width), kind),
        in_specs=[pl.BlockSpec(memory_space=pl.ANY)] * 3,
        out_specs=pl.BlockSpec(memory_space=pltpu.VMEM),
        scratch_shapes=[
            pltpu.VMEM((slots, 3, tokens, owners, width), kind),
            pltpu.VMEM((slots, 3, tokens * owners, width), jnp.float32),
            pltpu.VMEM((slots, owners, 3, tokens, width), kind),
            pltpu.VMEM((slots, size, 3, tokens, width), kind),
            pltpu.VMEM((slots, size, tokens, width), kind),
            pltpu.SemaphoreType.DMA((slots,)),
            pltpu.SemaphoreType.DMA,
            pltpu.SemaphoreType.DMA((slots,)),
            pltpu.SemaphoreType.DMA((2 * size // owners,)),
            pltpu.SemaphoreType.DMA,
            pltpu.SemaphoreType.DMA,
            pltpu.SemaphoreType.REGULAR,
        ],
        compiler_params=pltpu.CompilerParams(collective_id=0, has_side_effects=True),
    )(queries, keys, values)


def solution(mesh):
    return jax.shard_map(
        shards,
        mesh=mesh,
        in_specs=(
            P(("dp", "sp"), None, None),
            P(("dp", "sp"), None, None),
            P(("dp", "sp"), None, None),
        ),
        out_specs=P(("dp", "sp"), None),
        check_vma=False,
    )
```
